16 devices in a mesh: rep: 1, dp: 16 (over x, y, z, core).
Axes of the slice: x: 2, y: 2, z: 2, core: 2. Of those that a mesh axis runs over, the one named last changes fastest.
Arguments:
- x: bfloat16 [16, 2048, 896], P(('rep', 'dp'))
- dy: bfloat16 [16, 2048, 896], P(('rep', 'dp'))
- w_gate: bfloat16 [2, 896, 2304], replicated
- w_up: bfloat16 [2, 896, 2304], replicated
- w_down: bfloat16 [2, 2304, 896], replicated
- m_w_gate: float32 [2, 896, 2304], replicated
- m_w_up: float32 [2, 896, 2304], replicated
- m_w_down: float32 [2, 2304, 896], replicated
- v_w_gate: float32 [2, 896, 2304], replicated
- v_w_up: float32 [2, 896, 2304], replicated
- v_w_down: float32 [2, 2304, 896], replicated
Outputs:
- output 1: bfloat16 [2, 896, 2304], P('rep')
- output 2: bfloat16 [2, 896, 2304], P('rep')
- output 3: bfloat16 [2, 2304, 896], P('rep')
- output 4: float32 [2, 896, 2304], P('rep')
- output 5: float32 [2, 896, 2304], P('rep')
- output 6: float32 [2, 2304, 896], P('rep')
- output 7: float32 [2, 896, 2304], P('rep')
- output 8: float32 [2, 896, 2304], P('rep')
- output 9: float32 [2, 2304, 896], P('rep')
All inputs are finite; a program needn't handle non-finite values.
Results may differ from the reference program's by a relative error of at most 0.022.
Values are sent between devices in bfloat16 or wider.
A program may use at most 2.5 GiB of HBM per device.

```python
import jax
import jax.numpy as jnp
from jax import lax

SEQUENCES = 16
TOKENS = 2048
D = 896
FF = 2304
LAYERS = 2
NAMES = ("w_gate", "w_up", "w_down")
SHAPES = {"w_gate": (LAYERS, D, FF), "w_up": (LAYERS, D, FF), "w_down": (LAYERS, FF, D)}


def bump(key, n, height):
    away = (jnp.arange(n, dtype=jnp.int32) - jax.random.randint(key, (), 0, n, jnp.int32)) % n
    return jnp.where(away < n // 8, height, 1.0)


def together(key, own, strength):
    shared = jax.random.normal(key, own.shape[1:], jnp.float32)
    return (own + strength * shared) * lax.rsqrt(1 + strength * strength)


def setup_inputs(seed: int = 0, part: int = 0) -> dict:
    kx, kdy, ka, kb, kz, kf, kh, kl, *keys = jax.random.split(jax.random.key(seed), 8 + 3 * len(NAMES))
    kx, kdy, ka, kb = (jax.random.fold_in(k, part) for k in (kx, kdy, ka, kb))
    kw, km, kv = (keys[i::3] for i in range(3))
    shape = (SEQUENCES, TOKENS, D)
    much_x, much_dy = jax.random.uniform(kz, (2,), jnp.float32, 0.0, 1.0)
    loud = 2.0 ** jax.random.uniform(jax.random.fold_in(kz, 1), (), jnp.float32, -1.0, 2.0)
    layers = 2.0 ** jax.random.uniform(kl, (LAYERS, 1, 1), jnp.float32, -1.0, 1.0)
    x = together(ka, jax.random.normal(kx, shape, jnp.float32), much_x) * bump(kf, D, 4.0)
    dy = together(kb, jax.random.normal(kdy, shape, jnp.float32), much_dy)
    drawn = {"x": x.astype(jnp.bfloat16), "dy": (loud * dy * (SEQUENCES * TOKENS) ** -0.5).astype(jnp.bfloat16)}
    for key, name in zip(kw, NAMES, strict=True):
        w = jax.random.normal(key, SHAPES[name], jnp.float32) * SHAPES[name][1] ** -0.5
        drawn[name] = (w * {"w_gate": 1.0, "w_up": bump(kh, FF, 4.0), "w_down": layers}[name]).astype(jnp.bfloat16)
    for key, name in zip(km, NAMES, strict=True):
        drawn[f"m_{name}"] = 0.1 * jax.random.normal(key, SHAPES[name], jnp.float32)
    for key, name in zip(kv, NAMES, strict=True):
        drawn[f"v_{name}"] = jax.random.uniform(key, SHAPES[name], jnp.float32, 0.005, 0.015)
    return drawn


def matmul(a, w):
    return jnp.dot(a, w, preferred_element_type=jnp.float32).astype(jnp.bfloat16)


def normed(h):
    wide = h.astype(jnp.float32)
    scale = lax.rsqrt(jnp.mean(wide**2, -1, keepdims=True) + 1e-6)
    return (wide * scale).astype(jnp.bfloat16)


def layer(h, w):
    a = normed(h)
    gate = jnp.dot(a, w["w_gate"], preferred_element_type=jnp.float32)
    up = jnp.dot(a, w["w_up"], preferred_element_type=jnp.float32)
    return h + matmul((jax.nn.silu(gate) * up).astype(jnp.bfloat16), w["w_down"])


def adamw(w, m, v, g):
    m = 0.9 * m + 0.1 * g
    v = 0.95 * v + 0.05 * g * g
    step = m * lax.rsqrt(v + 1e-8) + 0.1 * w
    return (w - 0.02 * step).astype(jnp.bfloat16), m, v


def clipped(gradients, sum_of_squares, count):
    factor = jnp.minimum(1.0, 0.5 * lax.rsqrt(sum_of_squares / count + 1e-30))
    return [g * factor for g in gradients]


def stack(weights, h):
    return lax.scan(lambda h, w: (layer(h, w), None), h, weights)[0]


def reference(x, dy, w_gate, w_up, w_down, m_w_gate, m_w_up, m_w_down, v_w_gate, v_w_up, v_w_down):
    weights = dict(zip(NAMES, (w_gate, w_up, w_down), strict=True))

    def take(so_far, sequence):
        h, by_y = sequence
        _, back = jax.vjp(lambda w: stack(w, h), weights)
        return jax.tree.map(lambda total, term: total + term.astype(jnp.float32), so_far, back(by_y)[0]), None

    none_yet = {name: jnp.zeros(w.shape, jnp.float32) for name, w in weights.items()}
    by_weights, _ = lax.scan(take, none_yet, (x, dy))
    gradients = [by_weights[name].astype(jnp.bfloat16).astype(jnp.float32) for name in NAMES]
    gradients = clipped(gradients, sum(jnp.sum(g * g) for g in gradients), sum(g.size for g in gradients))
    new = [
        adamw(w.astype(jnp.float32), m, v, g)
        for w, m, v, g in zip((w_gate, w_up, w_down), (m_w_gate, m_w_up, m_w_down), (v_w_gate, v_w_up, v_w_down), gradients, strict=True)
    ]
    return tuple(one[which] for which in range(3) for one in new)
```

```python
import functools

import jax
import jax.numpy as jnp
from jax import lax
from jax.experimental import pallas as pl
from jax.experimental.pallas import tpu as pltpu
from jax.sharding import PartitionSpec as P

F32, BF16 = jnp.float32, jnp.bfloat16

LAYERS, T, D, FF = 2, 2048, 896, 2304
NC = 3
FC = FF // NC
RG, RD = D // 8, FC // 16
PANEL = (RG * FC // 2 // 128, 128)
TM = 512
STEPS = T // TM
ORDERS = ((3, 2, 1), (2, 1, 3), (1, 3, 2))
VMEM = 62 * 1024 * 1024


def dot(a, b, ca, cb):
    return lax.dot_general(a, b, (((ca,), (cb,)), ((), ())), preferred_element_type=F32)


def norm_scale(wide):
    return lax.rsqrt(jnp.mean(wide * wide, -1, keepdims=True) + 1e-6)


def normed(h):
    wide = h.astype(F32)
    return (wide * norm_scale(wide)).astype(BF16)


def once(shape, index):
    return pl.BlockSpec(shape, index, pipeline_mode=pl.Buffered(1))


def params(axes=1):
    return pltpu.CompilerParams(dimension_semantics=("arbitrary",) * axes, vmem_limit_bytes=VMEM)


def forward_body(x, wg, wu, wd, a, g, u, h1, a1):
    xv = x[...]
    av = normed(xv)
    a[...] = av
    gv = dot(av, wg[0], 1, 0)
    g[...] = gv
    uv = dot(av, wu[0], 1, 0)
    u[...] = uv
    p = (gv * jax.nn.sigmoid(gv) * uv).astype(BF16)
    hv = (xv.astype(F32) + dot(p, wd[0], 1, 0).astype(BF16).astype(F32)).astype(BF16)
    h1[...] = hv
    a1[...] = normed(hv)


def forward(x, wg, wu, wd):
    row = lambda n: pl.BlockSpec((TM, n), lambda i: (i, 0))
    whole = lambda s: once((1, *s), lambda i: (0, 0, 0))
    return pl.pallas_call(
        forward_body,
        grid=(STEPS,),
        in_specs=[row(D), whole((D, FF)), whole((D, FF)), whole((FF, D))],
        out_specs=[row(D), row(FF), row(FF), row(D), row(D)],
        out_shape=[jax.ShapeDtypeStruct((T, n), t) for n, t in ((D, BF16), (FF, F32), (FF, F32), (D, BF16), (D, BF16))],
        compiler_params=params(),
        cost_estimate=pl.CostEstimate(flops=6 * T * D * FF, bytes_accessed=70_000_000, transcendentals=0),
        name="fwd",
    )(x, wg, wu, wd)


def chunk_body(last_layer, a, dy, *refs):
    if last_layer:
        wg, wu, wd, out, dgo, duo, ag, au, ad = refs
    else:
        gr, ur, wd, out, ag, au, ad = refs
    i = pl.program_id(1)

    @pl.when(i == 0)
    def _():
        ag[...] = jnp.zeros_like(ag)
        au[...] = jnp.zeros_like(au)
        ad[...] = jnp.zeros_like(ad)

    av, dyv = a[...], dy[...]
    if last_layer:
        g = dot(av, wg[0], 1, 0)
        u = dot(av, wu[0], 1, 0)
    else:
        g, u = gr[...], ur[...]
    dp = dot(dyv, wd[0], 1, 1).astype(BF16).astype(F32)
    s = jax.nn.sigmoid(g)
    silu = g * s
    p = (silu * u).astype(BF16)
    du = (dp * silu).astype(BF16)
    dg = (dp * u * (s + silu * (1.0 - s))).astype(BF16)
    if last_layer:
        dgo[...] = dg
        duo[...] = du
    ad[...] += dot(p, dyv, 0, 0)
    ag[...] += dot(av, dg, 0, 0)
    au[...] += dot(av, du, 0, 0)

    @pl.when(i == STEPS - 1)
    def _():
        for c in range(2):
            for k in range(8):

                def put(m, at, value):
                    if last_layer:
                        out[2 * k + c, m, at, :] = value.astype(BF16)
                    else:
                        out[c, m, k, at, :] = value.astype(BF16)

                for m, acc in enumerate((ag, au)):
                    for q in range(3):
                        put(m, slice(q * RG, (q + 1) * RG), acc[k * RG : (k + 1) * RG, c * FC // 2 + q * 128 : c * FC // 2 + (q + 1) * 128])
                row = c * FC // 2 + k * RD
                for q in range(7):
                    put(2, slice(q * RD, (q + 1) * RD), ad[row : row + RD, q * 128 : (q + 1) * 128])


def backward(layer, a, dy, weights, gu=None):
    last = gu is None
    row = lambda n: pl.BlockSpec((TM, n), lambda j, i: (i, 0))
    tile = pl.BlockSpec((TM, FC), lambda j, i: (i, j))
    column = pl.BlockSpec((1, D, FC), lambda j, i: (layer, 0, j))
    rows = pl.BlockSpec((1, FC, D), lambda j, i: (layer, j, 0))
    if last:
        ins, in_specs = weights, [column, column, rows]
        out_specs = [once((16, 3, *PANEL), lambda j, i: (0, j, 0, 0)), tile, tile]
        out_shape = [jax.ShapeDtypeStruct((16, 9, *PANEL), BF16)] + [jax.ShapeDtypeStruct((T, FF), BF16)] * 2
    else:
        ins, in_specs = (*gu, weights[2]), [tile, tile, rows]
        out_specs = once((2, 3, 8, *PANEL), lambda j, i: (0, j, 0, 0, 0))
        out_shape = jax.ShapeDtypeStruct((2, 9, 8, *PANEL), BF16)
    return pl.pallas_call(
        functools.partial(chunk_body, last),
        grid=(NC, STEPS),
        in_specs=[row(D), row(D), *in_specs],
        out_specs=out_specs,
        out_shape=out_shape,
        scratch_shapes=[pltpu.VMEM((D, FC), F32), pltpu.VMEM((D, FC), F32), pltpu.VMEM((FC, D), F32)],
        compiler_params=params(2),
        cost_estimate=pl.CostEstimate(flops=(12 if last else 8) * T * D * FF, bytes_accessed=75_000_000, transcendentals=0),
        name=f"bwd{layer}",
    )(a, dy, *ins)


def input_body(dg, du, wg, wu, h, dy, out):
    by_gate = dot(dg[...], wg[0], 1, 1).astype(BF16).astype(F32)
    by_up = dot(du[...], wu[0], 1, 1).astype(BF16).astype(F32)
    ct = (by_gate + by_up).astype(BF16).astype(F32)
    wide = h[...].astype(F32)
    scale = norm_scale(wide)
    inner = jnp.sum(ct * wide, -1, keepdims=True)
    by_h = ct * scale - wide * (scale * scale * scale * inner * (1.0 / D))
    out[...] = (dy[...].astype(F32) + by_h.astype(BF16).astype(F32)).astype(BF16)


def input_gradient(dg, du, wg, wu, h, dy):
    row = lambda n: pl.BlockSpec((TM, n), lambda i: (i, 0))
    whole = once((1, D, FF), lambda i: (1, 0, 0))
    return pl.pallas_call(
        input_body,
        grid=(STEPS,),
        in_specs=[row(FF), row(FF), whole, whole, row(D), row(D)],
        out_specs=row(D),
        out_shape=jax.ShapeDtypeStruct((T, D), BF16),
        compiler_params=params(),
        cost_estimate=pl.CostEstimate(flops=4 * T * D * FF, bytes_accessed=40_000_000, transcendentals=0),
        name="bwd_in",
    )(dg, du, wg, wu, h, dy)


def reduce_body(g, r1, r0, factor, own, rb0, tot, sb1, rb1, sb2, rb2, sb3, rb3, part, nb, own_sem, core_sem, sem1, sem2, sem3, norm_sem):
    me = lax.axis_index("dp")
    base = {3: me // 8, 2: (me // 4) % 2, 1: (me // 2) % 2}
    core = me % 2
    partner = {b: me + (1 << b) * (1 - 2 * base[b]) for b in (1, 2, 3)}
    partner[0] = me + 1 - 2 * core

    def at(m, t):
        place = {b: 1 - base[b] if (t >> (2 - n)) & 1 else base[b] for n, b in enumerate(ORDERS[m])}
        return 4 * place[3] + 2 * place[2] + place[1]

    def send(src, dst, sems, piece, to):
        return pltpu.make_async_remote_copy(
            src_ref=src, dst_ref=dst, send_sem=sems.at[0, piece], recv_sem=sems.at[1, piece],
            device_id={"dp": to}, device_id_type=pl.DeviceIdType.MESH,
        )

    barrier = pltpu.get_barrier_semaphore()
    for d in range(1, 16):
        pl.semaphore_signal(barrier, inc=1, device_id={"dp": (me + d) % 16}, device_id_type=pl.DeviceIdType.MESH)
    pl.semaphore_wait(barrier, 15)

    def mine(p):
        return pltpu.make_async_copy(g.at[core, p], own.at[p], own_sem.at[p])

    def exchange(p):
        return send(g.at[1 - core, p], rb0.at[p], core_sem, p, partner[0])

    def first(p, m):
        return send(sb1.at[p], rb1.at[p], sem1, p, partner[ORDERS[m][0]])

    def second(p, m):
        return send(sb2.at[p], rb2.at[p], sem2, p, partner[ORDERS[m][1]])

    def third(p, m):
        return send(sb3.at[p], rb3.at[p], sem3, p, partner[ORDERS[m][2]])

    def each(body):
        def at_chunk(j, carry):
            for m in range(3):
                body(3 * j + m, m)
            return carry

        lax.fori_loop(0, NC, at_chunk, 0)

    def start(p, m):
        exchange(p).start()
        mine(p).start()

    each(start)

    def stage1(p, m):
        mine(p).wait()
        exchange(p).wait()
        for t in (4, 5, 6, 7, 0, 1, 2, 3):
            k = at(m, t)
            total = own[p, k].astype(F32) + rb0[p, k].astype(F32)
            if t >= 4:
                sb1[p, t - 4] = total.astype(BF16)
            else:
                tot[p, t] = total
        first(p, m).start()

    def stage2(p, m):
        first(p, m).wait()
        for t in (2, 3, 0, 1):
            total = tot[p, t] + rb1[p, t].astype(F32)
            if t >= 2:
                sb2[p, t - 2] = total.astype(BF16)
            else:
                tot[p, t] = total
        second(p, m).start()

    def stage3(p, m):
        second(p, m).wait()
        sb3[p, 0] = (tot[p, 1] + rb2[p, 1].astype(F32)).astype(BF16)
        tot[p, 0] = tot[p, 0] + rb2[p, 0].astype(F32)
        third(p, m).start()

    each(stage1)
    each(stage2)
    each(stage3)
    part[...] = jnp.zeros_like(part)

    def last(p, m):
        third(p, m).wait()
        r0[p] = (tot[p, 0] + rb3[p, 0].astype(F32)).astype(BF16)
        for r in (r0, r1):
            wide = r[p].astype(F32)
            part[...] += jnp.sum((wide * wide).reshape(PANEL[0] // 8, 8, 128), 0)

    each(last)

    def tell(d):
        return pltpu.make_async_remote_copy(
            src_ref=part, dst_ref=nb.at[me], send_sem=norm_sem.at[0, d], recv_sem=norm_sem.at[1, d],
            device_id={"dp": (me + d) % 16}, device_id_type=pl.DeviceIdType.MESH,
        )

    nb[me] = part[...]
    for d in range(1, 16):
        tell(d).start()
    for d in range(1, 16):
        tell(d).wait()
    total = nb[0]
    for d in range(1, 16):
        total += nb[d]
    squares = jnp.sum(jnp.sum(total, 0, keepdims=True), 1, keepdims=True)
    factor[...] = jnp.broadcast_to(jnp.minimum(1.0, 0.5 * lax.rsqrt(squares / (LAYERS * 3 * D * FF) + 1e-30)), factor.shape)


def reduce(g, r1):
    vmem = pl.BlockSpec(memory_space=pltpu.VMEM)
    buf = lambda n, t=BF16: pltpu.VMEM((9, n, *PANEL), t)
    dma = lambda *n: pltpu.SemaphoreType.DMA(n)
    return pl.pallas_call(
        reduce_body,
        in_specs=[pl.BlockSpec(memory_space=pl.ANY), vmem],
        out_specs=[vmem, vmem],
        out_shape=[jax.ShapeDtypeStruct((9, *PANEL), BF16), jax.ShapeDtypeStruct((8, 128), F32)],
        scratch_shapes=[
            buf(8), buf(8), buf(4, F32), buf(4), buf(4), buf(2), buf(2), buf(1), buf(1),
            pltpu.VMEM((8, 128), F32), pltpu.VMEM((16, 8, 128), F32),
            dma(9), dma(2, 9), dma(2, 9), dma(2, 9), dma(2, 9), dma(2, 16),
        ],
        compiler_params=pltpu.CompilerParams(collective_id=0, has_side_effects=True, vmem_limit_bytes=VMEM),
        cost_estimate=pl.CostEstimate(flops=30_000_000_000, bytes_accessed=20_000_000, transcendentals=0),
        name="reduce0",
    )(g, r1)


def adamw(w, m, v, g):
    m = 0.9 * m + 0.1 * g
    v = 0.95 * v + 0.05 * g * g
    step = m * lax.rsqrt(v + 1e-8) + 0.1 * w
    return (w - 0.02 * step).astype(BF16), m, v


def optimizer_body(factor, g, *refs):
    ins, outs = refs[:9], refs[-9:]
    f = factor[0:1, 0:1]
    for k in range(4):
        for m in range(3):
            w, mo, vo = (ins[n * 3 + m] for n in range(3))
            high = RG if m < 2 else RD
            rows = slice(k * high, (k + 1) * high)
            for q in range(PANEL[0] // high):
                cols = slice(q * 128, (q + 1) * 128)
                gq = g[k, 0, m, q * high : (q + 1) * high, :].astype(F32) * f
                new = adamw(w[0, rows, cols].astype(F32), mo[0, rows, cols], vo[0, rows, cols], gq)
                for n in range(3):
                    outs[n * 3 + m][0, rows, cols] = new[n]


def optimizer(layer, factor, gathered, state, so_far):
    column = pl.BlockSpec((1, D // 2, FC // 2), lambda j, c, r: (layer, r, 2 * j + c))
    rows = pl.BlockSpec((1, FC // 4, D), lambda j, c, r: (layer, 4 * j + 2 * c + r, 0))
    nine = [column, column, rows] * 3
    g = pl.BlockSpec((4, 1, 3, *PANEL), lambda j, c, r: (r, c, j, 0, 0))
    extra = [] if so_far is None else list(so_far)
    return pl.pallas_call(
        optimizer_body,
        grid=(NC, 2, 2),
        in_specs=[once((8, 128), lambda j, c, r: (0, 0)), g, *nine, *([pl.BlockSpec(memory_space=pl.ANY)] * len(extra))],
        out_specs=nine,
        out_shape=[jax.ShapeDtypeStruct(s.shape, s.dtype) for s in state],
        input_output_aliases={11 + n: n for n in range(len(extra))},
        compiler_params=params(3),
        cost_estimate=pl.CostEstimate(flops=15_000_000_000, bytes_accessed=137_000_000, transcendentals=0),
        name=f"adamw{layer}",
    )(factor, gathered.reshape(8, 2, 9, *PANEL), *state, *extra)


def solution(mesh):
    def step(x, dy, *state):
        x, dy = x[0], dy[0]
        weights = state[:3]
        a0, g0, u0, h1, a1 = forward(x, *weights)
        by_w1, dg, du = backward(1, a1, dy, weights)
        summed1 = lax.psum_scatter(by_w1, "dp", scatter_dimension=0)
        by_h = input_gradient(dg, du, weights[0], weights[1], h1, dy)
        by_w0 = backward(0, a0, by_h, weights, (g0, u0))
        summed1, by_w0 = lax.optimization_barrier((summed1, by_w0))
        all1 = lax.all_gather(summed1, "dp")
        summed0, factor = reduce(by_w0, summed1)
        all0 = lax.all_gather(summed0, "dp")
        new = optimizer(1, factor, all1, state, None)
        new = optimizer(0, factor, all0, state, new)
        return tuple(new)

    return jax.shard_map(
        step,
        mesh=mesh,
        in_specs=(P(("rep", "dp"), None, None),) * 2 + (P(None, None, None),) * 9,
        out_specs=(P("rep", None, None),) * 9,
        check_vma=False,
    )
```

```python
import functools

import jax
import jax.numpy as jnp
from jax import lax
from jax.experimental import pallas as pl
from jax.experimental.pallas import tpu as pltpu
from jax.sharding import PartitionSpec as P

F32, BF16 = jnp.float32, jnp.bfloat16

LAYERS, T, D, FF = 2, 2048, 896, 2304
FB = 256
NB = FF // FB
SPLIT = {1: 5, 0: 4}
TM = 512
RG = D // 8
PANEL = (RG, 128)
ORDERS = ((3, 2, 1), (2, 1, 3), (1, 3, 2))
MESH_ID = pl.DeviceIdType.MESH
VMEM = 62 * 1024 * 1024


def dot(a, b, ca, cb):
    return lax.dot_general(a, b, (((ca,), (cb,)), ((), ())), preferred_element_type=F32)


def norm_scale(wide):
    return lax.rsqrt(jnp.mean(wide * wide, -1, keepdims=True) + 1e-6)


def normed(h):
    wide = h.astype(F32)
    return (wide * norm_scale(wide)).astype(BF16)


def once(shape, index):
    return pl.BlockSpec(shape, index, pipeline_mode=pl.Buffered(1))


def params(**more):
    return pltpu.CompilerParams(dimension_semantics=("arbitrary",), vmem_limit_bytes=VMEM, **more)


def cost(flops, bytes_accessed):
    return pl.CostEstimate(flops=flops, bytes_accessed=bytes_accessed, transcendentals=0)


ANY = pl.BlockSpec(memory_space=pl.ANY)


def forward_body(x, dy, wg, wu, wd, at0, dyt, g, u, h1, a1, at1):
    xv = x[...]
    av = normed(xv)
    at0[...] = av.T
    dyt[...] = dy[...].T
    gv = dot(av, wg[0], 1, 0)
    g[...] = gv
    uv = dot(av, wu[0], 1, 0)
    u[...] = uv
    p = (gv * jax.nn.sigmoid(gv) * uv).astype(BF16)
    hv = (xv.astype(F32) + dot(p, wd[0], 1, 0).astype(BF16).astype(F32)).astype(BF16)
    h1[...] = hv
    av = normed(hv)
    a1[...] = av
    at1[...] = av.T


def forward(x, dy, wg, wu, wd):
    row = lambda n: pl.BlockSpec((TM, n), lambda i: (i, 0))
    col = pl.BlockSpec((D, TM), lambda i: (0, i))
    whole = lambda s: once((1, *s), lambda i: (0, 0, 0))
    flat = lambda a, b, t=BF16: jax.ShapeDtypeStruct((a, b), t)
    return pl.pallas_call(
        forward_body,
        grid=(T // TM,),
        in_specs=[row(D), row(D), whole((D, FF)), whole((D, FF)), whole((FF, D))],
        out_specs=[col, col, row(FF), row(FF), row(D), row(D), col],
        out_shape=[flat(D, T), flat(D, T), flat(T, FF, F32), flat(T, FF, F32), flat(T, D), flat(T, D), flat(D, T)],
        compiler_params=params(),
        cost_estimate=cost(6 * T * D * FF, 75_000_000),
        name="fwd",
    )(x, dy, wg, wu, wd)


class Reduction:
    def __init__(self, nb, g, scratch):
        self.nb, self.g = nb, g
        self.own, self.rb0, self.tot, self.sb1, self.rb1, self.sb2, self.rb2, self.sb3, self.rb3, self.own_sem, *self.sems = scratch
        self.me = me = lax.axis_index("dp")
        self.base = {3: me // 8, 2: (me // 4) % 2, 1: (me // 2) % 2}
        self.core = me % 2
        self.partner = {b: me + (1 << b) * (1 - 2 * self.base[b]) for b in (1, 2, 3)}
        self.partner[0] = me + 1 - 2 * self.core

    @staticmethod
    def scratch(nb):
        n = 3 * nb
        buf = lambda slabs, t=BF16: pltpu.VMEM((n, slabs, *PANEL), t)
        pair = pltpu.SemaphoreType.DMA((2, n))
        return [buf(8), buf(8), buf(4, F32), buf(4), buf(4), buf(2), buf(2), buf(1), buf(1), pltpu.SemaphoreType.DMA((n,)), pair, pair, pair, pair]

    def at(self, m, t):
        place = {b: 1 - self.base[b] if (t >> (2 - n)) & 1 else self.base[b] for n, b in enumerate(ORDERS[m])}
        return 4 * place[3] + 2 * place[2] + place[1]

    def send(self, stage, src, dst, p, to):
        sems = self.sems[stage]
        return pltpu.make_async_remote_copy(
            src_ref=src, dst_ref=dst, send_sem=sems.at[0, p], recv_sem=sems.at[1, p], device_id={"dp": self.partner[to]}, device_id_type=MESH_ID
        )

    def mine(self, p, m, b):
        return pltpu.make_async_copy(self.g.at[self.core, m, b], self.own.at[p], self.own_sem.at[p])

    def exchange(self, p, m, b):
        return self.send(0, self.g.at[1 - self.core, m, b], self.rb0.at[p], p, 0)

    def first(self, p, m):
        return self.send(1, self.sb1.at[p], self.rb1.at[p], p, ORDERS[m][0])

    def second(self, p, m):
        return self.send(2, self.sb2.at[p], self.rb2.at[p], p, ORDERS[m][1])

    def third(self, p, m):
        return self.send(3, self.sb3.at[p], self.rb3.at[p], p, ORDERS[m][2])

    def each(self, body):
        def at_block(b, carry):
            for m in range(3):
                body(3 * b + m, m, b)
            return carry

        lax.fori_loop(0, self.nb, at_block, 0)

    def barrier(self, everyone=False):
        others = [(self.me + d) % 16 for d in range(1, 16)] if everyone else [self.partner[b] for b in range(4)]
        semaphore = pltpu.get_barrier_semaphore()
        for other in others:
            pl.semaphore_signal(semaphore, inc=1, device_id={"dp": other}, device_id_type=MESH_ID)
        pl.semaphore_wait(semaphore, len(others))

    def start(self):
        def body(p, m, b):
            self.exchange(p, m, b).start()
            self.mine(p, m, b).start()

        self.each(body)

    def stage1(self):
        def body(p, m, b):
            self.mine(p, m, b).wait()
            self.exchange(p, m, b).wait()
            for t in (4, 5, 6, 7, 0, 1, 2, 3):
                k = self.at(m, t)
                total = self.own[p, k].astype(F32) + self.rb0[p, k].astype(F32)
                if t >= 4:
                    self.sb1[p, t - 4] = total.astype(BF16)
                else:
                    self.tot[p, t] = total
            self.first(p, m).start()

        self.each(body)

    def stage2(self):
        def body(p, m, b):
            self.first(p, m).wait()
            for t in (2, 3, 0, 1):
                total = self.tot[p, t] + self.rb1[p, t].astype(F32)
                if t >= 2:
                    self.sb2[p, t - 2] = total.astype(BF16)
                else:
                    self.tot[p, t] = total
            self.second(p, m).start()

        self.each(body)

    def stage3(self):
        def body(p, m, b):
            self.second(p, m).wait()
            self.sb3[p, 0] = (self.tot[p, 1] + self.rb2[p, 1].astype(F32)).astype(BF16)
            self.tot[p, 0] = self.tot[p, 0] + self.rb2[p, 0].astype(F32)
            self.third(p, m).start()

        self.each(body)

    def finish(self, r, at=0):
        def body(p, m, b):
            self.third(p, m).wait()
            r[m, at + b] = (self.tot[p, 0] + self.rb3[p, 0].astype(F32)).astype(BF16)

        self.each(body)

    def hooks(self, b, after, r, at=0):
        def before():
            @pl.when(b == 0)
            def _():
                self.barrier()
                self.start()

        def behind():
            for step in sorted(set(after)):

                @pl.when(b == step)
                def _():
                    for n, stage in enumerate((self.stage1, self.stage2, self.stage3, lambda: self.finish(r, at))):
                        if after[n] == step:
                            stage()

        return before, behind


def block_body(last, hook, *refs):
    refs = list(refs)
    take = lambda n: [refs.pop(0) for _ in range(n)]
    at, dyt, dy = take(3)
    a, wg, wu = take(3) if last else (None, None, None)
    gr, ur = take(2) if not last else (None, None)
    (wd,) = take(1)
    g_before = take(1)[0] if hook else None
    (out,) = take(1)
    dgo, duo = take(2) if last else (None, None)
    r = take(1)[0] if hook else None
    ps, dgs, dus, atv, dytv, sem = take(6)
    b = pl.program_id(0)
    if hook:
        before, behind = Reduction(hook[0], g_before, refs).hooks(b, hook[1], r)
        before()
    loads = pltpu.make_async_copy(at, atv, sem.at[0]), pltpu.make_async_copy(dyt, dytv, sem.at[1])

    @pl.when(b == 0)
    def _():
        for load in loads:
            load.start()

    for i in range(T // TM):
        rows = slice(i * TM, (i + 1) * TM)
        dp = dot(dy[rows, :], wd[0], 1, 1).astype(BF16).astype(F32)
        if last:
            g = dot(a[rows, :], wg[0], 1, 0)
            u = dot(a[rows, :], wu[0], 1, 0)
        else:
            g, u = gr[rows, :], ur[rows, :]
        s = jax.nn.sigmoid(g)
        silu = g * s
        ps[rows, :] = (silu * u).astype(BF16)
        du = (dp * silu).astype(BF16)
        dg = (dp * u * (s + silu * (1.0 - s))).astype(BF16)
        dgs[rows, :] = dg
        dus[rows, :] = du
        if last:
            dgo[rows, :] = dg
            duo[rows, :] = du

    @pl.when(b == 0)
    def _():
        for load in loads:
            load.wait()

    for m, (lhs, rhs) in enumerate(((atv, dgs), (atv, dus), (dytv, ps))):
        full = dot(lhs[...], rhs[...], 1, 0)
        for k in range(8):
            for c in range(2):
                out[c, m, 0, k] = full[k * RG : (k + 1) * RG, c * 128 : (c + 1) * 128].astype(BF16)
    if hook:
        behind()


def backward(layer, begin, n, at, dyt, dy, weights, a=None, gu=None, before=None, after=None):
    last = gu is None
    full = lambda s: once(s, lambda b: (0, 0))
    tile = pl.BlockSpec((T, FB), lambda b: (0, begin + b))
    column = pl.BlockSpec((1, D, FB), lambda b: (layer, 0, begin + b))
    rows = pl.BlockSpec((1, FB, D), lambda b: (layer, begin + b, 0))
    ins, in_specs = ((a, *weights), [full((T, D)), column, column, rows]) if last else ((*gu, weights[2]), [tile, tile, rows])
    out_specs = [pl.BlockSpec((2, 3, 1, 8, *PANEL), lambda b: (0, 0, b, 0, 0, 0))]
    out_shape = [jax.ShapeDtypeStruct((2, 3, n, 8, *PANEL), BF16)]
    if last:
        out_specs += [pl.BlockSpec((T, FB), lambda b: (0, b))] * 2
        out_shape += [jax.ShapeDtypeStruct((T, n * FB), BF16)] * 2
    scratch = [pltpu.VMEM((T, FB), BF16)] * 3 + [pltpu.VMEM((D, T), BF16)] * 2 + [pltpu.SemaphoreType.DMA((2,))]
    hook, more = None, {}
    if before is not None:
        nb = before.shape[2]
        hook, more = (nb, after), dict(collective_id=2 + layer, has_side_effects=True)
        ins, in_specs = (*ins, before), [*in_specs, ANY]
        out_specs.append(once((3, nb, *PANEL), lambda b: (0, 0, 0, 0)))
        out_shape.append(jax.ShapeDtypeStruct((3, nb, *PANEL), BF16))
        scratch += Reduction.scratch(nb)
    return pl.pallas_call(
        functools.partial(block_body, last, hook),
        grid=(n,),
        in_specs=[ANY, ANY, full((T, D)), *in_specs],
        out_specs=out_specs,
        out_shape=out_shape,
        scratch_shapes=scratch,
        compiler_params=params(**more),
        cost_estimate=cost((12 if last else 8) * T * D * FB * n, 8_000_000 * n),
        name=f"bwd{layer}{'ab'[hook is not None]}",
    )(at, dyt, dy, *ins)


def input_body(after, dga, dgb, dua, dub, wg, wu, h, dy, g_before, r_before, out, out_t, r, *scratch):
    b = pl.program_id(0)
    cut = dga.shape[1]
    nb = g_before.shape[2]
    before, behind = Reduction(nb, g_before, scratch).hooks(b, after, r, NB - nb)
    before()

    @pl.when(b == 0)
    def _():
        r[:, : NB - nb] = r_before[...]

    by_gate = dot(dga[...], wg[0, :, :cut], 1, 1) + dot(dgb[...], wg[0, :, cut:], 1, 1)
    by_up = dot(dua[...], wu[0, :, :cut], 1, 1) + dot(dub[...], wu[0, :, cut:], 1, 1)
    ct = (by_gate.astype(BF16).astype(F32) + by_up.astype(BF16).astype(F32)).astype(BF16).astype(F32)
    wide = h[...].astype(F32)
    scale = norm_scale(wide)
    inner = jnp.sum(ct * wide, -1, keepdims=True)
    by_h = ct * scale - wide * (scale * scale * scale * inner * (1.0 / D))
    new = (dy[...].astype(F32) + by_h.astype(BF16).astype(F32)).astype(BF16)
    out[...] = new
    out_t[...] = new.T
    behind()


def input_gradient(dgs, dus, wg, wu, h, dy, g_before, r_before, after):
    tm = 256
    row = lambda n: pl.BlockSpec((tm, n), lambda i: (i, 0))
    whole = once((1, D, FF), lambda i: (1, 0, 0))
    part = lambda n: once((3, n, *PANEL), lambda i: (0, 0, 0, 0))
    nb = g_before.shape[2]
    return pl.pallas_call(
        functools.partial(input_body, after),
        grid=(T // tm,),
        in_specs=[*(row(t.shape[1]) for t in (*dgs, *dus)), whole, whole, row(D), row(D), ANY, part(NB - nb)],
        out_specs=[row(D), pl.BlockSpec((D, tm), lambda i: (0, i)), part(NB)],
        out_shape=[jax.ShapeDtypeStruct(s, BF16) for s in ((T, D), (D, T), (3, NB, *PANEL))],
        scratch_shapes=Reduction.scratch(nb),
        compiler_params=params(collective_id=1, has_side_effects=True),
        cost_estimate=cost(4 * T * D * FF, 40_000_000),
        name="bwd_in",
    )(*dgs, *dus, wg, wu, h, dy, g_before, r_before)


def reduce_body(g, r_before, r1, r0, factor, part, nb, norm_sem, *scratch):
    blocks = g.shape[2]
    reduction = Reduction(blocks, g, scratch)
    me = reduction.me
    reduction.barrier(True)
    reduction.start()
    r0[:, : NB - blocks] = r_before[...]
    reduction.stage1()
    reduction.stage2()
    reduction.stage3()
    reduction.finish(r0, NB - blocks)
    part[...] = jnp.zeros_like(part)

    def squares(b, carry):
        for m in range(3):
            for r in (r0, r1):
                wide = r[m, b].astype(F32)
                part[...] += jnp.sum((wide * wide).reshape(RG // 8, 8, 128), 0)
        return carry

    lax.fori_loop(0, NB, squares, 0)

    def tell(d):
        return pltpu.make_async_remote_copy(
            src_ref=part, dst_ref=nb.at[me], send_sem=norm_sem.at[0, d], recv_sem=norm_sem.at[1, d],
            device_id={"dp": (me + d) % 16}, device_id_type=MESH_ID,
        )

    nb[me] = part[...]
    for d in range(1, 16):
        tell(d).start()
    for d in range(1, 16):
        tell(d).wait()
    total = nb[0]
    for d in range(1, 16):
        total += nb[d]
    total = jnp.sum(jnp.sum(total, 0, keepdims=True), 1, keepdims=True)
    factor[...] = jnp.broadcast_to(jnp.minimum(1.0, 0.5 * lax.rsqrt(total / (LAYERS * 3 * D * FF) + 1e-30)), factor.shape)


def reduce(g, r_before, r1):
    vmem = pl.BlockSpec(memory_space=pltpu.VMEM)
    return pl.pallas_call(
        reduce_body,
        in_specs=[ANY, vmem, vmem],
        out_specs=[vmem, vmem],
        out_shape=[jax.ShapeDtypeStruct((3, NB, *PANEL), BF16), jax.ShapeDtypeStruct((8, 128), F32)],
        scratch_shapes=[pltpu.VMEM((8, 128), F32), pltpu.VMEM((16, 8, 128), F32), pltpu.SemaphoreType.DMA((2, 16)), *Reduction.scratch(g.shape[2])],
        compiler_params=pltpu.CompilerParams(collective_id=0, has_side_effects=True, vmem_limit_bytes=VMEM),
        cost_estimate=cost(20_000_000_000, 20_000_000),
        name="reduce0",
    )(g, r_before, r1)


def adamw(w, m, v, g):
    m = 0.9 * m + 0.1 * g
    v = 0.95 * v + 0.05 * g * g
    step = m * lax.rsqrt(v + 1e-8) + 0.1 * w
    return (w - 0.02 * step).astype(BF16), m, v


def optimizer_body(factor, g, *refs):
    ins, outs = refs[:9], refs[-9:]
    f = factor[0:1, 0:1]
    for m in range(3):
        w, mo, vo = (ins[n * 3 + m] for n in range(3))
        for c in range(2):
            half = slice(c * 128, (c + 1) * 128)
            if m < 2:
                for k in range(8):
                    rows = slice(k * RG, (k + 1) * RG)
                    new = adamw(w[0, rows, half].astype(F32), mo[0, rows, half], vo[0, rows, half], g[k, c, m, 0].astype(F32) * f)
                    for n in range(3):
                        outs[n * 3 + m][0, rows, half] = new[n]
            else:
                turned = jnp.concatenate([g[k, c, m, 0].astype(F32) for k in range(8)], 0).T
                new = adamw(w[0, half, :].astype(F32), mo[0, half, :], vo[0, half, :], turned * f)
                for n in range(3):
                    outs[n * 3 + m][0, half, :] = new[n]


def optimizer(layer, factor, gathered, state, so_far):
    column = pl.BlockSpec((1, D, FB), lambda b: (layer, 0, b))
    rows = pl.BlockSpec((1, FB, D), lambda b: (layer, b, 0))
    nine = [column, column, rows] * 3
    g = pl.BlockSpec((8, 2, 3, 1, *PANEL), lambda b: (0, 0, 0, b, 0, 0))
    extra = [] if so_far is None else list(so_far)
    return pl.pallas_call(
        optimizer_body,
        grid=(NB,),
        in_specs=[once((8, 128), lambda b: (0, 0)), g, *nine, *([ANY] * len(extra))],
        out_specs=nine,
        out_shape=[jax.ShapeDtypeStruct(s.shape, s.dtype) for s in state],
        input_output_aliases={11 + n: n for n in range(len(extra))},
        compiler_params=params(),
        cost_estimate=cost(15_000_000_000, 137_000_000),
        name=f"adamw{layer}",
    )(factor, gathered.reshape(8, 2, 3, NB, *PANEL), *state, *extra)


def gather(part):
    return lax.all_gather(part.reshape(-1, *PANEL), "dp")


def solution(mesh):
    def step(x, dy, *state):
        x, dy = x[0], dy[0]
        weights = state[:3]
        at0, dyt, g0, u0, h1, a1, at1 = forward(x, dy, *weights)
        n = SPLIT[1]
        by1a, dga, dua = backward(1, 0, n, at1, dyt, dy, weights, a=a1)
        by1b, dgb, dub, r1a = backward(1, n, NB - n, at1, dyt, dy, weights, a=a1, before=by1a, after=(0, 2, 3, 3))
        by_h, by_ht, r1 = input_gradient((dga, dgb), (dua, dub), weights[0], weights[1], h1, dy, by1b, r1a, (1, 4, 6, 7))
        all1 = gather(r1)
        n = SPLIT[0]
        (by0a,) = backward(0, 0, n, at0, by_ht, by_h, weights, gu=(g0, u0))
        by0b, r0a = backward(0, n, NB - n, at0, by_ht, by_h, weights, gu=(g0, u0), before=by0a, after=(0, 2, 4, 4))
        r0, factor = reduce(by0b, r0a, r1)
        all0 = gather(r0)
        new = optimizer(1, factor, all1, state, None)
        new = optimizer(0, factor, all0, state, new)
        return tuple(new)

    return jax.shard_map(
        step,
        mesh=mesh,
        in_specs=(P(("rep", "dp"), None, None),) * 2 + (P(None, None, None),) * 9,
        out_specs=(P("rep", None, None),) * 9,
        check_vma=False,
    )
```

```python
import functools

import jax
import jax.numpy as jnp
from jax import lax
from jax.experimental import pallas as pl
from jax.experimental.pallas import tpu as pltpu
from jax.sharding import PartitionSpec as P

F32, BF16 = jnp.float32, jnp.bfloat16

LAYERS, T, D, FF = 2, 2048, 896, 2304
FB = 256
NB = FF // FB
SPLIT = 4
TM = 512
RG = D // 8
PANEL = (RG, 128)
ORDERS = ((3, 2, 1), (2, 1, 3), (1, 3, 2))
MESH_ID = pl.DeviceIdType.MESH
VMEM = 62 * 1024 * 1024


def dot(a, b, ca, cb):
    return lax.dot_general(a, b, (((ca,), (cb,)), ((), ())), preferred_element_type=F32)


def norm_scale(wide):
    return lax.rsqrt(jnp.mean(wide * wide, -1, keepdims=True) + 1e-6)


def normed(h):
    wide = h.astype(F32)
    return (wide * norm_scale(wide)).astype(BF16)


def once(shape, index):
    return pl.BlockSpec(shape, index, pipeline_mode=pl.Buffered(1))


def params(**more):
    return pltpu.CompilerParams(dimension_semantics=("arbitrary",), vmem_limit_bytes=VMEM, **more)


def cost(flops, bytes_accessed):
    return pl.CostEstimate(flops=flops, bytes_accessed=bytes_accessed, transcendentals=0)


ANY = pl.BlockSpec(memory_space=pl.ANY)


def forward_body(x, dy, wg, wu, wd, at0, dyt, g, u, h1, a1, at1):
    xv = x[...]
    av = normed(xv)
    at0[...] = av.T
    dyt[...] = dy[...].T
    gv = dot(av, wg[0], 1, 0)
    g[...] = gv
    uv = dot(av, wu[0], 1, 0)
    u[...] = uv
    p = (gv * jax.nn.sigmoid(gv) * uv).astype(BF16)
    hv = (xv.astype(F32) + dot(p, wd[0], 1, 0).astype(BF16).astype(F32)).astype(BF16)
    h1[...] = hv
    av = normed(hv)
    a1[...] = av
    at1[...] = av.T


def forward(x, dy, wg, wu, wd):
    row = lambda n: pl.BlockSpec((TM, n), lambda i: (i, 0))
    col = pl.BlockSpec((D, TM), lambda i: (0, i))
    whole = lambda s: once((1, *s), lambda i: (0, 0, 0))
    flat = lambda a, b, t=BF16: jax.ShapeDtypeStruct((a, b), t)
    return pl.pallas_call(
        forward_body,
        grid=(T // TM,),
        in_specs=[row(D), row(D), whole((D, FF)), whole((D, FF)), whole((FF, D))],
        out_specs=[col, col, row(FF), row(FF), row(D), row(D), col],
        out_shape=[flat(D, T), flat(D, T), flat(T, FF, F32), flat(T, FF, F32), flat(T, D), flat(T, D), flat(D, T)],
        compiler_params=params(),
        cost_estimate=cost(6 * T * D * FF, 75_000_000),
        name="fwd",
    )(x, dy, wg, wu, wd)


class Reduction:
    def __init__(self, nb, g, scratch):
        self.nb, self.g = nb, g
        self.own, self.rb0, self.tot, self.sb1, self.rb1, self.sb2, self.rb2, self.sb3, self.rb3, self.own_sem, *self.sems = scratch
        self.me = me = lax.axis_index("dp")
        self.base = {3: me // 8, 2: (me // 4) % 2, 1: (me // 2) % 2}
        self.core = me % 2
        self.partner = {b: me + (1 << b) * (1 - 2 * self.base[b]) for b in (1, 2, 3)}
        self.partner[0] = me + 1 - 2 * self.core

    @staticmethod
    def scratch(nb):
        n = 3 * nb
        buf = lambda slabs, t=BF16: pltpu.VMEM((n, slabs, *PANEL), t)
        pair = pltpu.SemaphoreType.DMA((2, n))
        return [buf(8), buf(8), buf(4, F32), buf(4), buf(4), buf(2), buf(2), buf(1), buf(1), pltpu.SemaphoreType.DMA((n,)), pair, pair, pair, pair]

    def at(self, m, t):
        place = {b: 1 - self.base[b] if (t >> (2 - n)) & 1 else self.base[b] for n, b in enumerate(ORDERS[m])}
        return 4 * place[3] + 2 * place[2] + place[1]

    def send(self, stage, src, dst, p, to):
        sems = self.sems[stage]
        return pltpu.make_async_remote_copy(
            src_ref=src, dst_ref=dst, send_sem=sems.at[0, p], recv_sem=sems.at[1, p], device_id={"dp": self.partner[to]}, device_id_type=MESH_ID
        )

    def mine(self, p, m, b):
        return pltpu.make_async_copy(self.g.at[self.core, m, b], self.own.at[p], self.own_sem.at[p])

    def exchange(self, p, m, b):
        return self.send(0, self.g.at[1 - self.core, m, b], self.rb0.at[p], p, 0)

    def first(self, p, m):
        return self.send(1, self.sb1.at[p], self.rb1.at[p], p, ORDERS[m][0])

    def second(self, p, m):
        return self.send(2, self.sb2.at[p], self.rb2.at[p], p, ORDERS[m][1])

    def third(self, p, m):
        return self.send(3, self.sb3.at[p], self.rb3.at[p], p, ORDERS[m][2])

    def each(self, body):
        def at_block(b, carry):
            for m in range(3):
                body(3 * b + m, m, b)
            return carry

        lax.fori_loop(0, self.nb, at_block, 0)

    def barrier(self, everyone=False):
        others = [(self.me + d) % 16 for d in range(1, 16)] if everyone else [self.partner[b] for b in range(4)]
        semaphore = pltpu.get_barrier_semaphore()
        for other in others:
            pl.semaphore_signal(semaphore, inc=1, device_id={"dp": other}, device_id_type=MESH_ID)
        pl.semaphore_wait(semaphore, len(others))

    def start(self):
        def body(p, m, b):
            self.exchange(p, m, b).start()
            self.mine(p, m, b).start()

        self.each(body)

    def stage1(self):
        def body(p, m, b):
            self.mine(p, m, b).wait()
            self.exchange(p, m, b).wait()
            for t in (4, 5, 6, 7, 0, 1, 2, 3):
                k = self.at(m, t)
                total = self.own[p, k].astype(F32) + self.rb0[p, k].astype(F32)
                if t >= 4:
                    self.sb1[p, t - 4] = total.astype(BF16)
                else:
                    self.tot[p, t] = total
            self.first(p, m).start()

        self.each(body)

    def stage2(self):
        def body(p, m, b):
            self.first(p, m).wait()
            for t in (2, 3, 0, 1):
                total = self.tot[p, t] + self.rb1[p, t].astype(F32)
                if t >= 2:
                    self.sb2[p, t - 2] = total.astype(BF16)
                else:
                    self.tot[p, t] = total
            self.second(p, m).start()

        self.each(body)

    def stage3(self):
        def body(p, m, b):
            self.second(p, m).wait()
            self.sb3[p, 0] = (self.tot[p, 1] + self.rb2[p, 1].astype(F32)).astype(BF16)
            self.tot[p, 0] = self.tot[p, 0] + self.rb2[p, 0].astype(F32)
            self.third(p, m).start()

        self.each(body)

    def finish(self, r, at=0):
        def body(p, m, b):
            self.third(p, m).wait()
            r[m, at + b] = (self.tot[p, 0] + self.rb3[p, 0].astype(F32)).astype(BF16)

        self.each(body)

    def hooks(self, b, after, r, at=0):
        def before():
            @pl.when(b == 0)
            def _():
                self.barrier()
                self.start()

        def behind():
            for step in sorted(set(after)):

                @pl.when(b == step)
                def _():
                    for n, stage in enumerate((self.stage1, self.stage2, self.stage3, lambda: self.finish(r, at))):
                        if after[n] == step:
                            stage()

        return before, behind


def block_body(last, hook, *refs):
    refs = list(refs)
    take = lambda n: [refs.pop(0) for _ in range(n)]
    at, dyt, dy = take(3)
    a, wg, wu = take(3) if last else (None, None, None)
    gr, ur = take(2) if not last else (None, None)
    (wd,) = take(1)
    g_before = take(1)[0] if hook else None
    (out,) = take(1)
    dgo, duo = take(2) if last else (None, None)
    r = take(1)[0] if hook else None
    ps, dgs, dus = take(3)
    b = pl.program_id(0)
    if hook:
        before, behind = Reduction(hook[0], g_before, refs).hooks(b, hook[1], r)
        before()
    for i in range(T // TM):
        rows = slice(i * TM, (i + 1) * TM)
        dp = dot(dy[rows, :], wd[0], 1, 1).astype(BF16).astype(F32)
        if last:
            g = dot(a[rows, :], wg[0], 1, 0)
            u = dot(a[rows, :], wu[0], 1, 0)
        else:
            g, u = gr[rows, :], ur[rows, :]
        s = jax.nn.sigmoid(g)
        silu = g * s
        ps[rows, :] = (silu * u).astype(BF16)
        du = (dp * silu).astype(BF16)
        dg = (dp * u * (s + silu * (1.0 - s))).astype(BF16)
        dgs[rows, :] = dg
        dus[rows, :] = du
        if last:
            dgo[rows, :] = dg
            duo[rows, :] = du

    for m, (lhs, rhs) in enumerate(((at, dgs), (at, dus), (dyt, ps))):
        full = dot(lhs[...], rhs[...], 1, 0)
        for k in range(8):
            for c in range(2):
                out[c, m, 0, k] = full[k * RG : (k + 1) * RG, c * 128 : (c + 1) * 128].astype(BF16)
    if hook:
        behind()


def backward(layer, begin, n, at, dyt, dy, weights, a=None, gu=None, before=None, after=None):
    last = gu is None
    full = lambda s: once(s, lambda b: (0, 0))
    tile = pl.BlockSpec((T, FB), lambda b: (0, begin + b))
    column = pl.BlockSpec((1, D, FB), lambda b: (layer, 0, begin + b))
    rows = pl.BlockSpec((1, FB, D), lambda b: (layer, begin + b, 0))
    ins, in_specs = ((a, *weights), [full((T, D)), column, column, rows]) if last else ((*gu, weights[2]), [tile, tile, rows])
    out_specs = [pl.BlockSpec((2, 3, 1, 8, *PANEL), lambda b: (0, 0, b, 0, 0, 0))]
    out_shape = [jax.ShapeDtypeStruct((2, 3, n, 8, *PANEL), BF16)]
    if last:
        out_specs += [pl.BlockSpec((T, FB), lambda b: (0, b))] * 2
        out_shape += [jax.ShapeDtypeStruct((T, n * FB), BF16)] * 2
    scratch = [pltpu.VMEM((T, FB), BF16)] * 3
    hook, more = None, {}
    if before is not None:
        nb = before.shape[2]
        hook, more = (nb, after), dict(collective_id=2 + layer, has_side_effects=True)
        ins, in_specs = (*ins, before), [*in_specs, ANY]
        out_specs.append(once((3, nb, *PANEL), lambda b: (0, 0, 0, 0)))
        out_shape.append(jax.ShapeDtypeStruct((3, nb, *PANEL), BF16))
        scratch += Reduction.scratch(nb)
    return pl.pallas_call(
        functools.partial(block_body, last, hook),
        grid=(n,),
        in_specs=[full((D, T)), full((D, T)), full((T, D)), *in_specs],
        out_specs=out_specs,
        out_shape=out_shape,
        scratch_shapes=scratch,
        compiler_params=params(**more),
        cost_estimate=cost((12 if last else 8) * T * D * FB * n, 8_000_000 * n),
        name=f"bwd{layer}{'ab'[hook is not None]}",
    )(at, dyt, dy, *ins)


def input_body(after, dga, dgb, dua, dub, wg, wu, h, dy, g_before, r_before, out, out_t, r, *scratch):
    b = pl.program_id(0)
    cut = dga.shape[1]
    nb = g_before.shape[2]
    before, behind = Reduction(nb, g_before, scratch).hooks(b, after, r, NB - nb)
    before()

    @pl.when(b == 0)
    def _():
        r[:, : NB - nb] = r_before[...]

    by_gate = dot(dga[...], wg[0, :, :cut], 1, 1) + dot(dgb[...], wg[0, :, cut:], 1, 1)
    by_up = dot(dua[...], wu[0, :, :cut], 1, 1) + dot(dub[...], wu[0, :, cut:], 1, 1)
    ct = (by_gate.astype(BF16).astype(F32) + by_up.astype(BF16).astype(F32)).astype(BF16).astype(F32)
    wide = h[...].astype(F32)
    scale = norm_scale(wide)
    inner = jnp.sum(ct * wide, -1, keepdims=True)
    by_h = ct * scale - wide * (scale * scale * scale * inner * (1.0 / D))
    new = (dy[...].astype(F32) + by_h.astype(BF16).astype(F32)).astype(BF16)
    out[...] = new
    out_t[...] = new.T
    behind()


def input_gradient(dgs, dus, wg, wu, h, dy, g_before, r_before, after):
    tm = 256
    row = lambda n: pl.BlockSpec((tm, n), lambda i: (i, 0))
    whole = once((1, D, FF), lambda i: (1, 0, 0))
    part = lambda n: once((3, n, *PANEL), lambda i: (0, 0, 0, 0))
    nb = g_before.shape[2]
    return pl.pallas_call(
        functools.partial(input_body, after),
        grid=(T // tm,),
        in_specs=[*(row(t.shape[1]) for t in (*dgs, *dus)), whole, whole, row(D), row(D), ANY, part(NB - nb)],
        out_specs=[row(D), pl.BlockSpec((D, tm), lambda i: (0, i)), part(NB)],
        out_shape=[jax.ShapeDtypeStruct(s, BF16) for s in ((T, D), (D, T), (3, NB, *PANEL))],
        scratch_shapes=Reduction.scratch(nb),
        compiler_params=params(collective_id=1, has_side_effects=True),
        cost_estimate=cost(4 * T * D * FF, 40_000_000),
        name="bwd_in",
    )(*dgs, *dus, wg, wu, h, dy, g_before, r_before)


def reduce_body(g, r1, r0, factor, part, nb, norm_sem, *scratch):
    reduction = Reduction(NB, g, scratch)
    me = reduction.me
    reduction.barrier(True)
    reduction.start()
    reduction.stage1()
    reduction.stage2()
    reduction.stage3()
    reduction.finish(r0)
    part[...] = jnp.zeros_like(part)

    def squares(b, carry):
        for m in range(3):
            for r in (r0, r1):
                wide = r[m, b].astype(F32)
                part[...] += jnp.sum((wide * wide).reshape(RG // 8, 8, 128), 0)
        return carry

    lax.fori_loop(0, NB, squares, 0)

    def tell(d):
        return pltpu.make_async_remote_copy(
            src_ref=part, dst_ref=nb.at[me], send_sem=norm_sem.at[0, d], recv_sem=norm_sem.at[1, d],
            device_id={"dp": (me + d) % 16}, device_id_type=MESH_ID,
        )

    nb[me] = part[...]
    for d in range(1, 16):
        tell(d).start()
    for d in range(1, 16):
        tell(d).wait()
    total = nb[0]
    for d in range(1, 16):
        total += nb[d]
    total = jnp.sum(jnp.sum(total, 0, keepdims=True), 1, keepdims=True)
    factor[...] = jnp.broadcast_to(jnp.minimum(1.0, 0.5 * lax.rsqrt(total / (LAYERS * 3 * D * FF) + 1e-30)), factor.shape)


def reduce(g, r1):
    vmem = pl.BlockSpec(memory_space=pltpu.VMEM)
    return pl.pallas_call(
        reduce_body,
        in_specs=[ANY, vmem],
        out_specs=[vmem, vmem],
        out_shape=[jax.ShapeDtypeStruct((3, NB, *PANEL), BF16), jax.ShapeDtypeStruct((8, 128), F32)],
        scratch_shapes=[pltpu.VMEM((8, 128), F32), pltpu.VMEM((16, 8, 128), F32), pltpu.SemaphoreType.DMA((2, 16)), *Reduction.scratch(NB)],
        compiler_params=pltpu.CompilerParams(collective_id=0, has_side_effects=True, vmem_limit_bytes=VMEM),
        cost_estimate=cost(20_000_000_000, 20_000_000),
        name="reduce0",
    )(g, r1)


def adamw(w, m, v, g):
    m = 0.9 * m + 0.1 * g
    v = 0.95 * v + 0.05 * g * g
    step = m * lax.rsqrt(v + 1e-8) + 0.1 * w
    return (w - 0.02 * step).astype(BF16), m, v


def optimizer_body(factor, g, *refs):
    ins, outs = refs[:9], refs[-9:]
    f = factor[0:1, 0:1]
    for m in range(3):
        w, mo, vo = (ins[n * 3 + m] for n in range(3))
        for c in range(2):
            half = slice(c * 128, (c + 1) * 128)
            if m < 2:
                for k in range(8):
                    rows = slice(k * RG, (k + 1) * RG)
                    new = adamw(w[0, rows, half].astype(F32), mo[0, rows, half], vo[0, rows, half], g[k, c, m, 0].astype(F32) * f)
                    for n in range(3):
                        outs[n * 3 + m][0, rows, half] = new[n]
            else:
                turned = jnp.concatenate([g[k, c, m, 0].astype(F32) for k in range(8)], 0).T
                new = adamw(w[0, half, :].astype(F32), mo[0, half, :], vo[0, half, :], turned * f)
                for n in range(3):
                    outs[n * 3 + m][0, half, :] = new[n]


def optimizer(layer, factor, gathered, state, so_far):
    column = pl.BlockSpec((1, D, FB), lambda b: (layer, 0, b))
    rows = pl.BlockSpec((1, FB, D), lambda b: (layer, b, 0))
    nine = [column, column, rows] * 3
    g = pl.BlockSpec((8, 2, 3, 1, *PANEL), lambda b: (0, 0, 0, b, 0, 0))
    extra = [] if so_far is None else list(so_far)
    return pl.pallas_call(
        optimizer_body,
        grid=(NB,),
        in_specs=[once((8, 128), lambda b: (0, 0)), g, *nine, *([ANY] * len(extra))],
        out_specs=nine,
        out_shape=[jax.ShapeDtypeStruct(s.shape, s.dtype) for s in state],
        input_output_aliases={11 + n: n for n in range(len(extra))},
        compiler_params=params(),
        cost_estimate=cost(15_000_000_000, 137_000_000),
        name=f"adamw{layer}",
    )(factor, gathered.reshape(8, 2, 3, NB, *PANEL), *state, *extra)


def gather(part):
    return lax.all_gather(part.reshape(-1, *PANEL), "dp")


def solution(mesh):
    def step(x, dy, *state):
        x, dy = x[0], dy[0]
        weights = state[:3]
        at0, dyt, g0, u0, h1, a1, at1 = forward(x, dy, *weights)
        n = SPLIT
        by1a, dga, dua = backward(1, 0, n, at1, dyt, dy, weights, a=a1)
        by1b, dgb, dub, r1a = backward(1, n, NB - n, at1, dyt, dy, weights, a=a1, before=by1a, after=(0, 2, 3, 4))
        by_h, by_ht, r1 = input_gradient((dga, dgb), (dua, dub), weights[0], weights[1], h1, dy, by1b, r1a, (1, 5, 7, 7))
        all1 = gather(r1)
        (by0,) = backward(0, 0, NB, at0, by_ht, by_h, weights, gu=(g0, u0))
        r0, factor = reduce(by0, r1)
        all0 = gather(r0)
        new = optimizer(1, factor, all1, state, None)
        new = optimizer(0, factor, all0, state, new)
        return tuple(new)

    return jax.shard_map(
        step,
        mesh=mesh,
        in_specs=(P(("rep", "dp"), None, None),) * 2 + (P(None, None, None),) * 9,
        out_specs=(P("rep", None, None),) * 9,
        check_vma=False,
    )
```
